32 devices in a mesh: patch: 16 (over z, y, x), col: 2 (over core).
Axes of the slice: x: 2, y: 2, z: 4, core: 2. Of those that a mesh axis runs over, the one named last changes fastest.
Arguments:
- density: float32 [4, 16384], P(None, 'patch'), may hold values from -6 to 6
- block_values: bfloat16 [64, 32, 256, 256], P('patch', 'col'), may hold values from -0.09375 to 0.09375
- block_rows: int32 [64, 32], P('patch', 'col'), may hold values from 0 to 63, as said below
- block_counts: int32 [64], P('patch'), may hold values from 1 to 32
Outputs:
- potential: float32 [4, 16384], P(None, 'patch')
The draws below stay inside these ranges and needn't reach their ends.
Inputs may be any that keep to these rules, and one draw needn't show every extreme that they name: `block_rows`: slots of a block column at or past its count are padding and are not part of the matrix. Block row r belongs to owner r // 4. The slots held by one device (block columns of one patch owner, one col index, live or padding) name block rows of distinct owners in groups of exactly 8 slots a group, so at most 8 of them fall on one owner.
All inputs are finite; a program needn't handle non-finite values.
Results may differ from the reference program's by a relative error of at most 0.0027.
Values sent between devices are 32-bit elements; how exact they have to be, the bound alone decides.
A program may use at most 64 MiB of HBM per device.

```python
import jax
import jax.numpy as jnp
from jax import lax

BS = 256
RHS = 4
LEVELS = 3
MAXB = 32
BLK_DEV = 4
NB = 64
NPANEL = 16384
CAP = 8
N_PATCH = 16
N_COL = 2


def draw_block_rows(key, part):
    slots = BLK_DEV * MAXB // N_COL
    devices = N_PATCH * N_COL
    keys = jax.random.split(jax.random.fold_in(key, 17), 3)
    owner_keys = jax.random.split(keys[0], devices)
    orders = jax.vmap(lambda sub: jax.random.permutation(sub, N_PATCH))(owner_keys)
    spot_keys = jax.random.split(keys[1], devices)
    spots = jax.vmap(lambda sub: jax.random.permutation(sub, slots))(spot_keys)
    groups = (spots // CAP).astype(jnp.int32)
    owners = jnp.take_along_axis(orders.astype(jnp.int32), groups, axis=1)
    within = jax.random.randint(keys[2], (devices, slots), 0, BLK_DEV, dtype=jnp.int32)
    rows = owners * BLK_DEV + within
    rows = rows.reshape(N_PATCH, N_COL, BLK_DEV, MAXB // N_COL).transpose(0, 2, 1, 3).reshape(NB, MAXB)
    return rows.astype(jnp.int32)


def with_ends(values, own_key, smallest, top_value):
    longest = values.shape.index(max(values.shape))
    spots = []
    for shift in (0, 1):
        where = [jax.random.randint(jax.random.fold_in(own_key, axis), (), 0, length) for axis, length in enumerate(values.shape)]
        where[longest] = (where[longest] + shift) % values.shape[longest]
        spots.append(tuple(where))
    return values.at[spots[0]].set(smallest).at[spots[1]].set(top_value)


def shard_levels(stream_key, shape, cuts, least, top_value):
    def one(position, blocks):
        draws = jax.random.uniform(jax.random.fold_in(jax.random.fold_in(stream_key, 6), position), (blocks,), jnp.float32, least / len(cuts), top_value / len(cuts))
        return jnp.repeat(jnp.exp(draws), shape[position] // blocks).reshape((-1,) + (1,) * (len(shape) - position - 1))

    level = one(*cuts[0])
    for cut in cuts[1:]:
        level = level * one(*cut)
    return level


def scatter_about(key, extent, deviation, most, cuts=(), kind=jnp.bfloat16):
    result = deviation * jax.random.normal(key, extent, jnp.float32)
    if cuts:
        result = result * shard_levels(key, extent, cuts, -0.22, 0.18)
    return jnp.clip(result, -most, most).astype(kind)


def setup_inputs(seed: int = 0) -> dict:
    splits = jax.random.split(jax.random.key(seed), 5)
    density = scatter_about(splits[0], (RHS, NPANEL), 1.0, 6.0, ((1, 16),), jnp.float32)
    block_values = scatter_about(splits[1], (NB, MAXB, BS, BS), (BS * MAXB // 2) ** -0.5, 0.09375, ((0, 16), (1, 2)))
    block_rows = draw_block_rows(jax.random.fold_in(splits[4], 71), 0)
    block_counts = with_ends(jax.random.randint(splits[3], (NB,), 1, MAXB + 1), jax.random.fold_in(splits[3], 1), 1, MAXB).astype(jnp.int32)
    return dict(density=density, block_values=block_values, block_rows=block_rows, block_counts=block_counts)


def forward_lift(density):
    smooth = density
    details = []
    for level_index in range(LEVELS):
        even_part = smooth[:, 0::2]
        odd_part = smooth[:, 1::2]
        zero_col = jnp.zeros_like(even_part[:, :1])
        even_next = jnp.concatenate([even_part[:, 1:], zero_col], axis=1)
        detail = odd_part - 0.5 * (even_part + even_next)
        detail_prior = jnp.concatenate([zero_col, detail[:, :-1]], axis=1)
        smooth = even_part + 0.25 * (detail_prior + detail)
        details.append(detail)
    return smooth, details


def owner_layout(pieces):
    parts = [piece.reshape(RHS, N_PATCH, -1) for piece in pieces]
    return jnp.concatenate(parts, axis=2).reshape(RHS, -1)


def inverse_lift(coefficients):
    local_len = BLK_DEV * BS
    local = coefficients.reshape(RHS, N_PATCH, local_len)
    coarse = local_len // (2 ** LEVELS)
    smooth = local[:, :, :coarse].reshape(RHS, -1)
    for level_index in range(LEVELS, 0, -1):
        lower = local_len // (2 ** level_index)
        upper = local_len // (2 ** (level_index - 1))
        detail = local[:, :, lower:upper].reshape(RHS, -1)
        zero_col = jnp.zeros_like(detail[:, :1])
        detail_prior = jnp.concatenate([zero_col, detail[:, :-1]], axis=1)
        even_part = smooth - 0.25 * (detail_prior + detail)
        even_next = jnp.concatenate([even_part[:, 1:], zero_col], axis=1)
        odd_part = detail + 0.5 * (even_part + even_next)
        smooth = jnp.stack([even_part, odd_part], axis=-1).reshape(RHS, -1)
    return smooth


def reference(density, block_values, block_rows, block_counts):
    smooth, details = forward_lift(density)
    coefficients = owner_layout([smooth] + details[::-1]).astype(jnp.bfloat16)
    blocks = coefficients.reshape(RHS, NB, BS).transpose(1, 0, 2)

    def apply_column(total, inputs):
        values, rows, count, vector = inputs
        terms = jnp.einsum("jkm,rm->jrk", values.astype(jnp.float32), vector.astype(jnp.float32), precision=lax.Precision.HIGHEST)
        live = (jnp.arange(MAXB, dtype=jnp.int32) < count).astype(jnp.float32)
        terms = terms * live[:, None, None]
        return total.at[rows].add(terms), None

    start = jnp.zeros((NB, RHS, BS), jnp.float32)
    applied, _ = lax.scan(apply_column, start, (block_values, block_rows, block_counts, blocks))
    flat = applied.transpose(1, 0, 2).reshape(RHS, -1)
    return 0.5 * density + inverse_lift(flat)
```

```python
import functools

import jax
import jax.numpy as jnp
import numpy as np
from jax import lax
from jax.experimental import pallas as pl
from jax.experimental.pallas import tpu as pltpu
from jax.sharding import PartitionSpec as P

LEVELS = 3
LANES = 128
GROUP = 4
MESH = pl.DeviceIdType.MESH


def np_forward(x):
    smooth, details = x, []
    for _ in range(LEVELS):
        even, odd = smooth[:, 0::2], smooth[:, 1::2]
        zero = np.zeros_like(even[:, :1])
        detail = odd - 0.5 * (even + np.concatenate([even[:, 1:], zero], 1))
        smooth = even + 0.25 * (np.concatenate([zero, detail[:, :-1]], 1) + detail)
        details.append(detail)
    return [smooth] + details[::-1]


def np_inverse(pieces):
    smooth = pieces[0]
    for detail in pieces[1:]:
        zero = np.zeros_like(detail[:, :1])
        even = smooth - 0.25 * (np.concatenate([zero, detail[:, :-1]], 1) + detail)
        odd = detail + 0.5 * (even + np.concatenate([even[:, 1:], zero], 1))
        smooth = np.stack([even, odd], -1).reshape(even.shape[0], -1)
    return smooth


def piece_widths(window):
    return [window >> LEVELS] + [window >> level for level in range(LEVELS, 0, -1)]


def forward_matrix(window):
    widths = piece_widths(window)

    def middle(count, at):
        parts = np_forward(np.eye(count * window))
        return np.concatenate([part[:, at * w:(at + 1) * w] for part, w in zip(parts, widths)], 1)

    inner = middle(5, 2)[2 * window - LANES:3 * window + LANES]
    first = middle(5, 0)[:window] - inner[LANES:-LANES]
    last = middle(5, 4)[4 * window:] - inner[LANES:-LANES]
    half = LANES // 2
    result = inner.copy()
    assert not result[:half].any() and not result[-half:].any()
    result[:half] = first[:half]
    result[-half:] = last[-half:]
    assert not first[half:].any() and not last[:-half].any()
    return result


def inverse_matrix(window):
    widths = piece_widths(window)
    count, at = 5, 2
    starts = np.cumsum([0] + widths)

    def response(piece, index):
        pieces = [np.zeros((1, count * w)) for w in widths]
        pieces[piece][0, index] = 1.0
        return np_inverse(pieces)[0, at * window:(at + 1) * window]

    result = np.zeros((3 * window, window))
    for piece, width in enumerate(widths):
        for k in range(width):
            result[starts[piece] + k] = response(piece, at * width + k)
    for piece, width in enumerate(widths):
        if piece:
            result[window + starts[piece] + width - 1] = response(piece, at * width - 1)
        result[window + starts[piece]] += response(piece, (at + 1) * width)
    base = 2 * window
    for row, piece, side in (
        (LANES - 1, 1, -1), (2 * LANES - 1, 2, -1), (2 * LANES - 2, 3, -1),
        (0, 0, 1), (2, 1, 1), (LANES, 2, 1), (1, 3, 1),
    ):
        width = widths[piece]
        result[base + row] = response(piece, at * width - 1 if side < 0 else (at + 1) * width)
    return result


def as_bf16(matrix):
    exact = np.asarray(matrix, dtype=jnp.bfloat16)
    assert (exact.astype(np.float64) == matrix).all()
    return exact


def thirds(value):
    high = value.astype(jnp.bfloat16)
    rest = value - high.astype(jnp.float32)
    middle = rest.astype(jnp.bfloat16)
    low = (rest - middle.astype(jnp.float32)).astype(jnp.bfloat16)
    return jnp.concatenate([high, middle, low], axis=0)


def split_dot(value, matrix):
    rows = value.shape[0]
    out = jnp.dot(thirds(value), matrix, preferred_element_type=jnp.float32)
    return out[:rows] + out[rows:2 * rows] + out[2 * rows:]


def kernel(owners, sides, col_blocks, slots, block, rows_ref, counts_ref, density_ref, values_ref, fwd_ref, inv_ref,
           out_ref, held, fwd, inv, vec, acc, recv, halo, halo_recv, left_in, right_in, mine, other,
           value_sem, fwd_sem, inv_sem, edge_send, edge_recv, send_sem, recv_sem, halo_send_sem, halo_recv_sem, col_sem):
    me = lax.axis_index("patch")
    core = lax.axis_index("col")
    local_len = col_blocks * block
    tall = col_blocks * sides
    groups_per_col = slots // GROUP
    groups = col_blocks * groups_per_col
    windows = local_len // block

    def value_copy(g):
        c = g // groups_per_col
        j = (g % groups_per_col) * GROUP
        return pltpu.make_async_copy(values_ref.at[c, pl.ds(j, GROUP)], held.at[c, pl.ds(j, GROUP)], value_sem.at[g])

    fwd_copy = pltpu.make_async_copy(fwd_ref, fwd, fwd_sem)
    inv_copy = pltpu.make_async_copy(inv_ref, inv, inv_sem)
    fwd_copy.start()

    @pl.loop(0, groups)
    def _(g):
        value_copy(g).start()

    inv_copy.start()

    barrier = pltpu.get_barrier_semaphore()

    @pl.loop(1, owners)
    def _(k):
        pl.semaphore_signal(barrier, inc=1, device_id=(lax.rem(me + k, owners), core), device_id_type=MESH)

    pl.semaphore_signal(barrier, inc=1, device_id=(me, 1 - core), device_id_type=MESH)
    pl.semaphore_wait(barrier, owners)

    to_next = pltpu.make_async_remote_copy(
        src_ref=density_ref.at[:, pl.ds(local_len - LANES, LANES)], dst_ref=left_in,
        send_sem=edge_send.at[0], recv_sem=edge_recv.at[0],
        device_id=(lax.rem(me + 1, owners), core), device_id_type=MESH)
    to_prev = pltpu.make_async_remote_copy(
        src_ref=density_ref.at[:, pl.ds(0, LANES)], dst_ref=right_in,
        send_sem=edge_send.at[1], recv_sem=edge_recv.at[1],
        device_id=(lax.rem(me + owners - 1, owners), core), device_id_type=MESH)

    @pl.when(me < owners - 1)
    def _():
        to_next.start()

    @pl.when(me > 0)
    def _():
        to_prev.start()

    acc[...] = jnp.zeros_like(acc)

    @pl.when(me == 0)
    def _():
        left_in[...] = jnp.zeros_like(left_in)

    @pl.when(me == owners - 1)
    def _():
        right_in[...] = jnp.zeros_like(right_in)

    @pl.when(me > 0)
    def _():
        to_next.wait_recv()

    @pl.when(me < owners - 1)
    def _():
        to_prev.wait_recv()

    lane = lax.broadcasted_iota(jnp.int32, (sides, LANES), 1)
    half = LANES // 2
    density = density_ref[...]
    before = jnp.where(
        lane < half,
        jnp.where(me == 0, density[:, :LANES], 0.0),
        left_in[...])
    after = jnp.where(
        lane >= half,
        jnp.where(me == owners - 1, density[:, local_len - LANES:], 0.0),
        right_in[...])
    rows_in = []
    for w in range(windows):
        start, stop = w * block, (w + 1) * block
        left = before if w == 0 else jnp.where(lane >= half, density[:, start - LANES:start], 0.0)
        right = after if w == windows - 1 else jnp.where(lane < half, density[:, stop:stop + LANES], 0.0)
        rows_in.append(jnp.concatenate([left, density[:, start:stop], right], axis=1))
    fwd_in = jnp.concatenate(rows_in, axis=0)
    fwd_copy.wait()
    lifted = split_dot(fwd_in, fwd[...])
    heads = [lifted[w * sides:(w + 1) * sides, :LANES] for w in range(windows)]
    fine = [lifted[w * sides:(w + 1) * sides, LANES:] for w in range(windows)]

    def turned(value, shift):
        shift = shift % LANES
        return pltpu.roll(value, shift, 1) if shift else value

    quarter = LANES // 4
    smooth = turned(heads[0], 0)
    coarse = turned(heads[0], -quarter)
    for w in range(1, windows):
        inside = lane >= w * quarter
        smooth = jnp.where(inside, turned(heads[w], w * quarter), smooth)
        coarse = jnp.where(inside, turned(heads[w], (w - 1) * quarter), coarse)
    mid = [jnp.where(lane < half, turned(heads[2 * i], half), heads[2 * i + 1]) for i in range(windows // 2)]
    tiles = [smooth, coarse] + mid + fine
    for c in range(col_blocks):
        rounded = jnp.concatenate(tiles[2 * c:2 * c + 2], axis=1).astype(jnp.bfloat16).astype(jnp.float32)
        vec[c] = jnp.concatenate([rounded] * (8 // sides), axis=0)

    height = min(256, acc.shape[0])
    steps = acc.shape[0] // height
    shift = sides.bit_length() - 1
    key = jnp.right_shift(lax.broadcasted_iota(jnp.int32, (height // 8, 8, block), 0) * 8
                          + lax.broadcasted_iota(jnp.int32, (height // 8, 8, block), 1), shift)
    first_slot = core * slots

    def apply_group(g, carry):
        value_copy(g).wait()
        c = g // groups_per_col
        j0 = (g % groups_per_col) * GROUP
        x8 = vec[c]
        targets = []
        for u in range(GROUP):
            alive = first_slot + j0 + u < counts_ref[c]
            targets.append(jnp.where(alive, rows_ref[c, j0 + u], -1))

        def part(step):
            total = acc[pl.ds(step * height, height), :]
            for u in range(GROUP):
                hit = key == targets[u] - step * (height // sides)
                left = jnp.where(hit, x8[None], 0.0).reshape(height, block).astype(jnp.bfloat16)
                total = total + lax.dot_general(left, held[c, j0 + u], (((1,), (1,)), ((), ())),
                                                preferred_element_type=jnp.float32)
            acc[pl.ds(step * height, height), :] = total

        if steps == 1:
            part(0)
        else:
            pl.loop(0, steps)(part)
        return carry

    lax.fori_loop(0, groups, apply_group, 0)

    def main_copy(k, there):
        return pltpu.make_async_remote_copy(
            src_ref=acc.at[pl.ds(there * tall, tall), :], dst_ref=recv.at[me],
            send_sem=send_sem.at[k], recv_sem=recv_sem.at[me],
            device_id=(there, core), device_id_type=MESH)

    def halo_copy(k, there):
        return pltpu.make_async_remote_copy(
            src_ref=halo.at[there], dst_ref=halo_recv.at[me],
            send_sem=halo_send_sem.at[k], recv_sem=halo_recv_sem.at[me],
            device_id=(there, core), device_id_type=MESH)

    @pl.loop(1, owners)
    def _(k):
        main_copy(k, lax.rem(me + k, owners)).start()

    lane8 = lax.broadcasted_iota(jnp.int32, (8, LANES), 1)

    def pack(there):
        prev = acc[pl.ds(jnp.maximum(there - 1, 0) * tall, tall), LANES:]
        nxt = acc[pl.ds(jnp.minimum(there + 1, owners - 1) * tall, tall), :]
        tile = jnp.where(lane8 == LANES - 1, prev[:8], pltpu.roll(prev[8:], LANES - 1, 1))
        tile = jnp.where(lane8 == 0, nxt[:8, :LANES], tile)
        tile = jnp.where(lane8 == 1, pltpu.roll(nxt[8:, :LANES], 1, 1), tile)
        halo[there] = jnp.where(lane8 == 2, pltpu.roll(nxt[:8, LANES:], 2, 1), tile)

    @pl.loop(1, owners)
    def _(k):
        there = lax.rem(me + k, owners)
        pack(there)
        halo_copy(k, there).start()

    pack(me)

    def arrive(k, carry):
        total, edge = carry
        source = lax.rem(me + owners - k, owners)
        pltpu.make_async_remote_copy(
            src_ref=recv.at[source], dst_ref=recv.at[source], send_sem=send_sem.at[k], recv_sem=recv_sem.at[source],
            device_id=(source, core), device_id_type=MESH).wait_recv()
        pltpu.make_async_remote_copy(
            src_ref=halo_recv.at[source], dst_ref=halo_recv.at[source], send_sem=halo_send_sem.at[k],
            recv_sem=halo_recv_sem.at[source], device_id=(source, core), device_id_type=MESH).wait_recv()
        return total + recv[source], edge + halo_recv[source]

    total, edge = lax.fori_loop(
        1, owners, arrive, (acc[pl.ds(me * tall, tall), :], halo[me]))
    mine[:tall] = total
    mine[tall:, :LANES] = edge
    mine[tall:, LANES:] = jnp.zeros_like(edge)
    swap = pltpu.make_async_remote_copy(
        src_ref=mine, dst_ref=other, send_sem=col_sem.at[0], recv_sem=col_sem.at[1],
        device_id=(me, 1 - core), device_id_type=MESH)
    swap.start()

    @pl.loop(1, owners)
    def _(k):
        there = lax.rem(me + k, owners)
        main_copy(k, there).wait_send()
        halo_copy(k, there).wait_send()

    @pl.when(me < owners - 1)
    def _():
        to_next.wait_send()

    @pl.when(me > 0)
    def _():
        to_prev.wait_send()

    inv_copy.wait()
    swap.wait()
    full = mine[...] + other[...]
    total, edge = full[:tall], full[tall:, :LANES]

    def tile(c, side):
        return total[c * sides:(c + 1) * sides, side * LANES:(side + 1) * LANES]

    smooth, coarse = tile(0, 0), tile(0, 1)
    mid = [tile(1, 0), tile(1, 1)]
    fine = [tile(2 + w // 2, w % 2) for w in range(windows)]
    heads = []
    for w in range(windows):
        piece = turned(mid[w // 2], half if w % 2 == 0 else 0)
        piece = jnp.where(lane < half, turned(coarse, quarter - w * quarter), piece)
        heads.append(jnp.where(lane < quarter, turned(smooth, -w * quarter), piece))
    zero = jnp.zeros((sides, LANES), jnp.float32)
    last_tiles = (
        jnp.where(lane == 2, -turned(coarse, 3), jnp.where(lane == 1, -turned(fine[-1], 2), 0.0)),
        jnp.where(lane == 0, -turned(mid[1], 1), 0.0),
    )
    pieces = []
    for w in range(windows):
        head_near = zero
        fine_near = zero
        if w > 0:
            head_near = jnp.where((lane == half - 1) | (lane == LANES - 1), heads[w - 1], head_near)
            fine_near = jnp.where(lane == LANES - 1, fine[w - 1], fine_near)
        if w < windows - 1:
            head_near = jnp.where((lane == 0) | (lane == quarter) | (lane == half), heads[w + 1], head_near)
            fine_near = jnp.where(lane == 0, fine[w + 1], fine_near)
        ends = [zero, zero]
        for i in range(2):
            arrived = edge[i * sides:(i + 1) * sides]
            if w == 0:
                ends[i] = jnp.where((lane >= half) & (me > 0), arrived, ends[i])
            if w == windows - 1:
                ends[i] = jnp.where(lane < half, jnp.where(me == owners - 1, last_tiles[i], arrived), ends[i])
        pieces.append(jnp.concatenate([heads[w], fine[w], head_near, fine_near] + ends, axis=1))
    rebuilt = split_dot(jnp.concatenate(pieces, axis=0), inv[...])
    for w in range(windows):
        at = pl.ds(w * block, block)
        out_ref[:, at] = 0.5 * density_ref[:, at] + rebuilt[w * sides:(w + 1) * sides]


def body(owners, fwd, inv, density, block_values, block_rows, block_counts):
    sides, local_len = density.shape
    col_blocks, slots, block, _ = block_values.shape
    tall = col_blocks * sides
    f32, bf16 = jnp.float32, jnp.bfloat16
    vmem = pl.BlockSpec(memory_space=pltpu.VMEM)
    smem = pl.BlockSpec(memory_space=pltpu.SMEM)
    hbm = pl.BlockSpec(memory_space=pl.ANY)
    dma = pltpu.SemaphoreType.DMA
    return pl.pallas_call(
        functools.partial(kernel, owners, sides, col_blocks, slots, block),
        out_shape=jax.ShapeDtypeStruct(density.shape, f32),
        in_specs=[smem, smem, vmem, hbm, hbm, hbm],
        out_specs=vmem,
        scratch_shapes=[
            pltpu.VMEM(block_values.shape, bf16),
            pltpu.VMEM(fwd.shape, bf16),
            pltpu.VMEM(inv.shape, bf16),
            pltpu.VMEM((col_blocks, 8, block), f32),
            pltpu.VMEM((owners * tall, block), f32),
            pltpu.VMEM((owners, tall, block), f32),
            pltpu.VMEM((owners, 8, LANES), f32),
            pltpu.VMEM((owners, 8, LANES), f32),
            pltpu.VMEM((sides, LANES), f32),
            pltpu.VMEM((sides, LANES), f32),
            pltpu.VMEM((tall + 8, block), f32),
            pltpu.VMEM((tall + 8, block), f32),
            dma((col_blocks * slots // GROUP,)),
            dma, dma, dma((2,)), dma((2,)),
            dma((owners,)), dma((owners,)), dma((owners,)), dma((owners,)),
            dma((2,)),
        ],
        compiler_params=pltpu.CompilerParams(
            collective_id=0, has_side_effects=True, vmem_limit_bytes=60 * 1024 * 1024),
    )(block_rows, block_counts, density, block_values, jnp.asarray(fwd), jnp.asarray(inv))


def solution(mesh):
    owners = mesh.shape["patch"]
    window = 2 * LANES
    fwd, inv = as_bf16(forward_matrix(window)), as_bf16(inverse_matrix(window))
    return jax.shard_map(
        functools.partial(body, owners, fwd, inv),
        mesh=mesh,
        in_specs=(P(None, "patch"), P("patch", "col", None, None), P("patch", "col"), P("patch")),
        out_specs=P(None, "patch"),
        check_vma=False,
    )
```

```python
import functools

import jax
import jax.numpy as jnp
import numpy as np
from jax import lax
from jax.experimental import pallas as pl
from jax.experimental.pallas import tpu as pltpu
from jax.sharding import PartitionSpec as P

LEVELS = 3
LANES = 128
GROUP = 8
MESH = pl.DeviceIdType.MESH


def np_forward(x):
    smooth, details = x, []
    for _ in range(LEVELS):
        even, odd = smooth[:, 0::2], smooth[:, 1::2]
        zero = np.zeros_like(even[:, :1])
        detail = odd - 0.5 * (even + np.concatenate([even[:, 1:], zero], 1))
        smooth = even + 0.25 * (np.concatenate([zero, detail[:, :-1]], 1) + detail)
        details.append(detail)
    return [smooth] + details[::-1]


def np_inverse(pieces):
    smooth = pieces[0]
    for detail in pieces[1:]:
        zero = np.zeros_like(detail[:, :1])
        even = smooth - 0.25 * (np.concatenate([zero, detail[:, :-1]], 1) + detail)
        odd = detail + 0.5 * (even + np.concatenate([even[:, 1:], zero], 1))
        smooth = np.stack([even, odd], -1).reshape(even.shape[0], -1)
    return smooth


def piece_widths(window):
    return [window >> LEVELS] + [window >> level for level in range(LEVELS, 0, -1)]


def forward_matrix(window):
    widths = piece_widths(window)

    def middle(count, at):
        parts = np_forward(np.eye(count * window))
        return np.concatenate([part[:, at * w:(at + 1) * w] for part, w in zip(parts, widths)], 1)

    inner = middle(5, 2)[2 * window - LANES:3 * window + LANES]
    first = middle(5, 0)[:window] - inner[LANES:-LANES]
    last = middle(5, 4)[4 * window:] - inner[LANES:-LANES]
    half = LANES // 2
    result = inner.copy()
    assert not result[:half].any() and not result[-half:].any()
    result[:half] = first[:half]
    result[-half:] = last[-half:]
    assert not first[half:].any() and not last[:-half].any()
    return result


def inverse_matrix(window):
    widths = piece_widths(window)
    count, at = 5, 2
    starts = np.cumsum([0] + widths)

    def response(piece, index):
        pieces = [np.zeros((1, count * w)) for w in widths]
        pieces[piece][0, index] = 1.0
        return np_inverse(pieces)[0, at * window:(at + 1) * window]

    result = np.zeros((3 * window, window))
    for piece, width in enumerate(widths):
        for k in range(width):
            result[starts[piece] + k] = response(piece, at * width + k)
    for piece, width in enumerate(widths):
        if piece:
            result[window + starts[piece] + width - 1] = response(piece, at * width - 1)
        result[window + starts[piece]] += response(piece, (at + 1) * width)
    base = 2 * window
    for row, piece, side in (
        (LANES - 1, 1, -1), (2 * LANES - 1, 2, -1), (2 * LANES - 2, 3, -1),
        (0, 0, 1), (2, 1, 1), (LANES, 2, 1), (1, 3, 1),
    ):
        width = widths[piece]
        result[base + row] = response(piece, at * width - 1 if side < 0 else (at + 1) * width)
    return result


def as_bf16(matrix):
    exact = np.asarray(matrix, dtype=jnp.bfloat16)
    assert (exact.astype(np.float64) == matrix).all()
    return exact


def thirds(value):
    high = value.astype(jnp.bfloat16)
    rest = value - high.astype(jnp.float32)
    middle = rest.astype(jnp.bfloat16)
    low = (rest - middle.astype(jnp.float32)).astype(jnp.bfloat16)
    return jnp.concatenate([high, middle, low], axis=0)


def split_dot(value, matrix):
    rows = value.shape[0]
    out = jnp.dot(thirds(value), matrix, preferred_element_type=jnp.float32)
    return out[:rows] + out[rows:2 * rows] + out[2 * rows:]


def kernel(owners, sides, col_blocks, slots, block, rows_ref, counts_ref, density_ref, values_ref, fwd_ref, inv_ref,
           out_ref, held, fwd, inv, vec, terms, acc, recv, halo, side_in, left_in, right_in, mine, other,
           value_sem, fwd_sem, inv_sem, edge_send, edge_recv, send_sem, recv_sem, side_send, side_recv, col_sem):
    me = lax.axis_index("patch")
    core = lax.axis_index("col")
    local_len = col_blocks * block
    tall = col_blocks * sides
    groups_per_col = slots // GROUP
    groups = col_blocks * groups_per_col
    windows = local_len // block

    def value_copy(g):
        c = g // groups_per_col
        j = (g % groups_per_col) * GROUP
        return pltpu.make_async_copy(values_ref.at[c, pl.ds(j, GROUP)], held.at[c, pl.ds(j, GROUP)], value_sem.at[g])

    fwd_copy = pltpu.make_async_copy(fwd_ref, fwd, fwd_sem)
    inv_copy = pltpu.make_async_copy(inv_ref, inv, inv_sem)
    fwd_copy.start()

    early = col_blocks // 2
    for c in [early] + [c for c in range(col_blocks) if c != early]:
        for i in range(groups_per_col):
            value_copy(c * groups_per_col + i).start()

    inv_copy.start()

    barrier = pltpu.get_barrier_semaphore()

    @pl.loop(1, owners)
    def _(k):
        pl.semaphore_signal(barrier, inc=1, device_id=(lax.rem(me + k, owners), core), device_id_type=MESH)

    pl.semaphore_signal(barrier, inc=1, device_id=(me, 1 - core), device_id_type=MESH)

    for k in (1, owners - 1):
        pl.semaphore_signal(barrier, inc=1, device_id=(lax.rem(me + k, owners), 1 - core), device_id_type=MESH)


    to_next = pltpu.make_async_remote_copy(
        src_ref=density_ref.at[:, pl.ds(local_len - LANES, LANES)], dst_ref=left_in,
        send_sem=edge_send.at[0], recv_sem=edge_recv.at[0],
        device_id=(lax.rem(me + 1, owners), core), device_id_type=MESH)
    to_prev = pltpu.make_async_remote_copy(
        src_ref=density_ref.at[:, pl.ds(0, LANES)], dst_ref=right_in,
        send_sem=edge_send.at[1], recv_sem=edge_recv.at[1],
        device_id=(lax.rem(me + owners - 1, owners), core), device_id_type=MESH)

    lane = lax.broadcasted_iota(jnp.int32, (sides, LANES), 1)
    half = LANES // 2
    quarter = LANES // 4
    density = density_ref[...]

    def turned(value, shift):
        shift = shift % LANES
        return pltpu.roll(value, shift, 1) if shift else value

    def lift(from_left, from_right):
        before = jnp.where(lane < half, jnp.where(me == 0, density[:, :LANES], 0.0), from_left)
        after = jnp.where(lane >= half, jnp.where(me == owners - 1, density[:, local_len - LANES:], 0.0), from_right)
        rows_in = []
        for w in range(windows):
            start, stop = w * block, (w + 1) * block
            left = before if w == 0 else jnp.where(lane >= half, density[:, start - LANES:start], 0.0)
            right = after if w == windows - 1 else jnp.where(lane < half, density[:, stop:stop + LANES], 0.0)
            rows_in.append(jnp.concatenate([left, density[:, start:stop], right], axis=1))
        lifted = split_dot(jnp.concatenate(rows_in, axis=0), fwd[...])
        heads = [lifted[w * sides:(w + 1) * sides, :LANES] for w in range(windows)]
        fine = [lifted[w * sides:(w + 1) * sides, LANES:] for w in range(windows)]
        smooth = turned(heads[0], 0)
        coarse = turned(heads[0], -quarter)
        for w in range(1, windows):
            inside = lane >= w * quarter
            smooth = jnp.where(inside, turned(heads[w], w * quarter), smooth)
            coarse = jnp.where(inside, turned(heads[w], (w - 1) * quarter), coarse)
        mid = [jnp.where(lane < half, turned(heads[2 * i], half), heads[2 * i + 1]) for i in range(windows // 2)]
        return [smooth, coarse] + mid + fine

    def place(tiles, c):
        column = jnp.concatenate(tiles[2 * c:2 * c + 2], axis=1)
        vec[c] = jnp.concatenate([column] * (LANES // sides), axis=0).astype(jnp.bfloat16)

    shift = sides.bit_length() - 1
    lane_slot = jnp.right_shift(lax.broadcasted_iota(jnp.int32, (block, LANES), 1), shift)

    def apply_column(c):
        at = c * slots * sides
        here = pl.ds(at // LANES * LANES, LANES)
        first = at % LANES // sides
        found = terms[:, here]
        for i in range(0, groups_per_col):
            value_copy(c * groups_per_col + i).wait()
        for i in range(0, slots, GROUP):
            got = lax.dot_general(held[c, i:i + GROUP].reshape(GROUP * block, block), vec[c],
                                  (((1,), (1,)), ((), ())), preferred_element_type=jnp.float32)
            for u in range(GROUP):
                found = jnp.where(lane_slot == first + i + u, got[u * block:(u + 1) * block], found)
        terms[:, here] = found

    terms[...] = jnp.zeros_like(terms)
    fwd_copy.wait()
    place(lift(jnp.zeros((sides, LANES), jnp.float32), jnp.zeros((sides, LANES), jnp.float32)), early)
    apply_column(early)

    pl.semaphore_wait(barrier, owners + 2)

    @pl.when(me < owners - 1)
    def _():
        to_next.start()

    @pl.when(me > 0)
    def _():
        to_prev.start()

    @pl.when(me == 0)
    def _():
        left_in[...] = jnp.zeros_like(left_in)
        side_in[0] = jnp.zeros_like(side_in[0])

    @pl.when(me == owners - 1)
    def _():
        right_in[...] = jnp.zeros_like(right_in)
        side_in[1] = jnp.zeros_like(side_in[1])

    width = terms.shape[1]
    first_slot = core * slots
    column_key = lax.broadcasted_iota(jnp.int32, (8, width), 1)
    column_slot = jnp.right_shift(column_key, shift)
    wanted = jnp.full((8, width), -1, jnp.int32)
    for c in range(col_blocks):
        count = counts_ref[c]
        for j in range(slots):
            row = jnp.where(first_slot + j < count, rows_ref[c, j], -1)
            wanted = jnp.where(column_slot == c * slots + j, row, wanted)
    wanted = wanted * sides + jnp.bitwise_and(column_key, sides - 1)
    height = min(256, acc.shape[0])
    row_key = (lax.broadcasted_iota(jnp.int32, (height // 8, 8, width), 0) * 8
               + lax.broadcasted_iota(jnp.int32, (height // 8, 8, width), 1))

    @pl.when(me > 0)
    def _():
        to_next.wait_recv()

    @pl.when(me < owners - 1)
    def _():
        to_prev.wait_recv()

    tiles = lift(left_in[...], right_in[...])
    later = [c for c in range(col_blocks) if c != early]
    for c in later:
        place(tiles, c)
    for c in later:
        apply_column(c)

    split = thirds(terms[...])

    def scatter(step):
        chosen = jnp.where(row_key == wanted[None] - step * height, 1.0, 0.0).reshape(height, width).astype(jnp.bfloat16)
        total = jnp.zeros((height, block), jnp.float32)
        for i in range(3):
            total = total + lax.dot_general(chosen, split[i * block:(i + 1) * block], (((1,), (1,)), ((), ())),
                                            preferred_element_type=jnp.float32)
        acc[pl.ds(step * height, height), :] = total

    if acc.shape[0] == height:
        scatter(0)
    else:
        pl.loop(0, acc.shape[0] // height)(scatter)

    def main_copy(k, there):
        return pltpu.make_async_remote_copy(
            src_ref=acc.at[pl.ds(there * tall, tall), :], dst_ref=recv.at[me],
            send_sem=send_sem.at[k], recv_sem=recv_sem.at[me],
            device_id=(there, core), device_id_type=MESH)

    def side_copies(to_left):
        side = 1 if to_left else 0
        there = jnp.maximum(me - 1, 0) if to_left else jnp.minimum(me + 1, owners - 1)
        return [pltpu.make_async_remote_copy(
            src_ref=halo, dst_ref=side_in.at[side, core], send_sem=side_send.at[side, to],
            recv_sem=side_recv.at[side, core], device_id=(there, to), device_id_type=MESH) for to in range(2)]

    def side_arrived(side):
        for source in range(2):
            pltpu.make_async_remote_copy(
                src_ref=halo, dst_ref=side_in.at[side, source], send_sem=side_send.at[side, source],
                recv_sem=side_recv.at[side, source], device_id=(me, 1 - core), device_id_type=MESH).wait_recv()

    @pl.loop(1, owners)
    def _(k):
        main_copy(k, lax.rem(me + k, owners)).start()

    def arrive(k, total):
        source = lax.rem(me + owners - k, owners)
        pltpu.make_async_remote_copy(
            src_ref=recv.at[source], dst_ref=recv.at[source], send_sem=send_sem.at[k], recv_sem=recv_sem.at[source],
            device_id=(source, core), device_id_type=MESH).wait_recv()
        return total + recv[source]

    total = lax.fori_loop(1, owners, arrive, acc[pl.ds(me * tall, tall), :])
    mine[...] = total
    lane8 = lax.broadcasted_iota(jnp.int32, (8, LANES), 1)
    edge = jnp.where(lane8 == LANES - 1, total[:8, LANES:], pltpu.roll(total[8:, LANES:], LANES - 1, 1))
    edge = jnp.where(lane8 == 0, total[:8, :LANES], edge)
    edge = jnp.where(lane8 == 1, pltpu.roll(total[8:, :LANES], 1, 1), edge)
    halo[...] = jnp.where(lane8 == 2, pltpu.roll(total[:8, LANES:], 2, 1), edge)

    @pl.when(me < owners - 1)
    def _():
        for copy in side_copies(False):
            copy.start()

    @pl.when(me > 0)
    def _():
        for copy in side_copies(True):
            copy.start()

    swap = pltpu.make_async_remote_copy(
        src_ref=mine, dst_ref=other, send_sem=col_sem.at[0], recv_sem=col_sem.at[1],
        device_id=(me, 1 - core), device_id_type=MESH)
    swap.start()

    @pl.loop(1, owners)
    def _(k):
        there = lax.rem(me + k, owners)
        main_copy(k, there).wait_send()

    @pl.when(me < owners - 1)
    def _():
        to_next.wait_send()
        for copy in side_copies(False):
            copy.wait_send()

    @pl.when(me > 0)
    def _():
        to_prev.wait_send()
        for copy in side_copies(True):
            copy.wait_send()

    inv_copy.wait()
    swap.wait()
    total = mine[...] + other[...]

    @pl.when(me > 0)
    def _():
        side_arrived(0)

    @pl.when(me < owners - 1)
    def _():
        side_arrived(1)

    edge = jnp.where(lane8 >= LANES // 2, side_in[0, 0] + side_in[0, 1], side_in[1, 0] + side_in[1, 1])

    def tile(c, side):
        return total[c * sides:(c + 1) * sides, side * LANES:(side + 1) * LANES]

    smooth, coarse = tile(0, 0), tile(0, 1)
    mid = [tile(1, 0), tile(1, 1)]
    fine = [tile(2 + w // 2, w % 2) for w in range(windows)]
    heads = []
    for w in range(windows):
        piece = turned(mid[w // 2], half if w % 2 == 0 else 0)
        piece = jnp.where(lane < half, turned(coarse, quarter - w * quarter), piece)
        heads.append(jnp.where(lane < quarter, turned(smooth, -w * quarter), piece))
    zero = jnp.zeros((sides, LANES), jnp.float32)
    last_tiles = (
        jnp.where(lane == 2, -turned(coarse, 3), jnp.where(lane == 1, -turned(fine[-1], 2), 0.0)),
        jnp.where(lane == 0, -turned(mid[1], 1), 0.0),
    )
    pieces = []
    for w in range(windows):
        head_near = zero
        fine_near = zero
        if w > 0:
            head_near = jnp.where((lane == half - 1) | (lane == LANES - 1), heads[w - 1], head_near)
            fine_near = jnp.where(lane == LANES - 1, fine[w - 1], fine_near)
        if w < windows - 1:
            head_near = jnp.where((lane == 0) | (lane == quarter) | (lane == half), heads[w + 1], head_near)
            fine_near = jnp.where(lane == 0, fine[w + 1], fine_near)
        ends = [zero, zero]
        for i in range(2):
            arrived = edge[i * sides:(i + 1) * sides]
            if w == 0:
                ends[i] = jnp.where((lane >= half) & (me > 0), arrived, ends[i])
            if w == windows - 1:
                ends[i] = jnp.where(lane < half, jnp.where(me == owners - 1, last_tiles[i], arrived), ends[i])
        pieces.append(jnp.concatenate([heads[w], fine[w], head_near, fine_near] + ends, axis=1))
    rebuilt = split_dot(jnp.concatenate(pieces, axis=0), inv[...])
    for w in range(windows):
        at = pl.ds(w * block, block)
        out_ref[:, at] = 0.5 * density_ref[:, at] + rebuilt[w * sides:(w + 1) * sides]


def body(owners, fwd, inv, density, block_values, block_rows, block_counts):
    sides, local_len = density.shape
    col_blocks, slots, block, _ = block_values.shape
    tall = col_blocks * sides
    f32, bf16 = jnp.float32, jnp.bfloat16
    vmem = pl.BlockSpec(memory_space=pltpu.VMEM)
    smem = pl.BlockSpec(memory_space=pltpu.SMEM)
    hbm = pl.BlockSpec(memory_space=pl.ANY)
    dma = pltpu.SemaphoreType.DMA
    return pl.pallas_call(
        functools.partial(kernel, owners, sides, col_blocks, slots, block),
        out_shape=jax.ShapeDtypeStruct(density.shape, f32),
        in_specs=[smem, smem, vmem, hbm, hbm, hbm],
        out_specs=vmem,
        scratch_shapes=[
            pltpu.VMEM(block_values.shape, bf16),
            pltpu.VMEM(fwd.shape, bf16),
            pltpu.VMEM(inv.shape, bf16),
            pltpu.VMEM((col_blocks, LANES, block), bf16),
            pltpu.VMEM((block, col_blocks * slots * sides), f32),
            pltpu.VMEM((owners * tall, block), f32),
            pltpu.VMEM((owners, tall, block), f32),
            pltpu.VMEM((8, LANES), f32),
            pltpu.VMEM((2, 2, 8, LANES), f32),
            pltpu.VMEM((sides, LANES), f32),
            pltpu.VMEM((sides, LANES), f32),
            pltpu.VMEM((tall, block), f32),
            pltpu.VMEM((tall, block), f32),
            dma((col_blocks * slots // GROUP,)),
            dma, dma, dma((2,)), dma((2,)),
            dma((owners,)), dma((owners,)), dma((2, 2)), dma((2, 2)),
            dma((2,)),
        ],
        compiler_params=pltpu.CompilerParams(
            collective_id=0, has_side_effects=True, vmem_limit_bytes=60 * 1024 * 1024),
    )(block_rows, block_counts, density, block_values, jnp.asarray(fwd), jnp.asarray(inv))


def solution(mesh):
    owners = mesh.shape["patch"]
    window = 2 * LANES
    fwd, inv = as_bf16(forward_matrix(window)), as_bf16(inverse_matrix(window))
    return jax.shard_map(
        functools.partial(body, owners, fwd, inv),
        mesh=mesh,
        in_specs=(P(None, "patch"), P("patch", "col", None, None), P("patch", "col"), P("patch")),
        out_specs=P(None, "patch"),
        check_vma=False,
    )
```
